256 devices in a mesh: dom: 32 (over y, z), slab: 8 (over x, core).
Axes of the slice: x: 4, y: 4, z: 8, core: 2. Of those that a mesh axis runs over, the one named last changes fastest.
Arguments:
- particles: bfloat16 [6144, 32, 1024], P('dom', 'slab'), may hold values from -6 to 6
- refs: bfloat16 [2048, 32, 2048], P('dom', 'slab'), may hold values from -6 to 6
- orient: int32 [6144], P('dom'), may hold values from 0 to 2047, as said below
- shifts: int32 [6144, 8, 2], P('dom'), may hold values from -4 to 4
- tilt: int32 [6144], P('dom'), may hold values from 0 to 15
- wedge: float32 [16, 32, 1024], P(None, 'slab'), may hold values from 0.1 to 1
Outputs:
- new_refs: float32 [2048, 32, 2048], P('dom', 'slab')
- shift_weights: float32 [6144, 8], P('dom')
The draws below stay inside these ranges and needn't reach their ends.
Inputs may be any that keep to these rules, and one draw needn't show every extreme that they name: `orient`: split the particles into aligned blocks of 192 (the rows of one device) and the orientations into ranges of 64. In every block at most 12 particles have orientations in any one range, and in every draw one range holds exactly 12 particles of every block.
All inputs are finite; a program needn't handle non-finite values.
Results may differ from the reference program's by a relative error of at most 0.004.
Values may be sent and summed in bfloat16 or wider, within the bound.
A program may use at most 128 MiB of HBM per device.

```python
import math
import jax
import jax.numpy as jnp
from jax import lax

BOX = 32
ORIENT = 2048
TILTS = 16
NSHIFT = 8
P_DEV = 192
PARTICLES = 6144
ORIENT_DEV = 64
CAP = 12
N_DOM = 32


def draw_orient(key, part):
    pool_size = N_DOM * CAP
    full_owner = jax.random.randint(jax.random.fold_in(key, 7), (), 0, N_DOM)
    pool = jnp.arange(pool_size, dtype=jnp.int32) // CAP
    position = jnp.arange(pool_size, dtype=jnp.int32)

    def one_block(block_key):
        key_one, key_two, key_three, key_four = jax.random.split(block_key, 4)
        ranks = jax.random.permutation(key_one, pool_size).astype(jnp.int32)
        priority = jnp.where(pool == full_owner, position - pool_size, ranks)
        order = jnp.argsort(priority)
        owners = pool[order[:P_DEV]]
        owners = jax.random.permutation(key_two, owners)
        left = jax.random.randint(key_three, (P_DEV,), 0, ORIENT_DEV)
        right = jax.random.randint(key_four, (P_DEV,), 0, ORIENT_DEV)
        local = jnp.maximum(left, right)
        return owners * ORIENT_DEV + local
    keys = jax.random.split(jax.random.fold_in(key, 11), N_DOM)
    return jax.vmap(one_block)(keys).reshape(-1).astype(jnp.int32)


def set_ends(result, key, least, high):
    longest = result.shape.index(max(result.shape))
    spots = []
    for shift in (0, 1):
        where = [jax.random.randint(jax.random.fold_in(key, axis), (), 0, length) for axis, length in enumerate(result.shape)]
        where[longest] = (where[longest] + shift) % result.shape[longest]
        spots.append(tuple(where))
    return result.at[spots[0]].set(least).at[spots[1]].set(high)


def block_scale(key, extent, cuts, smallest, top_value):
    level = 1.0
    for dim, blocks in cuts:
        draws = jax.random.uniform(jax.random.fold_in(jax.random.fold_in(key, 6), dim), (blocks,), jnp.float32, smallest / len(cuts), top_value / len(cuts))
        level = level * jnp.repeat(jnp.exp(draws), extent[dim] // blocks).reshape((-1,) + (1,) * (len(extent) - 1 - dim))
    return level


def scatter_about(stream_key, dims, deviation, limit, pieces=(), kind=jnp.bfloat16):
    entries = jax.random.normal(stream_key, dims, jnp.float32) * deviation
    if len(pieces) > 0:
        entries = block_scale(stream_key, dims, pieces, -0.22, 0.18) * entries
    return jnp.clip(entries, min=-limit, max=limit).astype(kind)


def setup_inputs(seed: int = 0) -> dict:
    key_list = jax.random.split(jax.random.key(seed), 7)
    particles = scatter_about(key_list[0], (PARTICLES, BOX, BOX * BOX), 1.0, 6.0, ((0, 32), (1, 8)))
    refs = scatter_about(key_list[1], (ORIENT, BOX, 2 * BOX * BOX), 1.0, 6.0, ((0, 32), (1, 8)))
    orient = draw_orient(jax.random.fold_in(key_list[6], 71), 0)
    shifts = set_ends(jax.random.randint(key_list[3], (PARTICLES, NSHIFT, 2), -4, 5), jax.random.fold_in(key_list[3], 1), -4, 4).astype(jnp.int32)
    tilt = set_ends(jax.random.randint(key_list[4], (PARTICLES,), 0, TILTS), jax.random.fold_in(key_list[4], 1), 0, TILTS - 1).astype(jnp.int32)
    wedge = jnp.clip(0.1 + 0.9 * jax.random.uniform(key_list[5], (TILTS, BOX, BOX * BOX), jnp.float32) ** block_scale(key_list[5], (TILTS, BOX, BOX * BOX), ((1, 8),), -0.2, 0.2), 0.1, 1.0)
    return dict(particles=particles, refs=refs, orient=orient, shifts=shifts, tilt=tilt, wedge=wedge)


def dft_table(box):
    pixel = jnp.arange(box * box, dtype=jnp.int32)
    row_y = pixel // box
    row_x = pixel % box
    phase = (row_y[:, None] * row_y[None, :] + row_x[:, None] * row_x[None, :]) % box
    angle = phase.astype(jnp.float32) * (2.0 * math.pi / box)
    return jnp.concatenate([jnp.cos(angle), -jnp.sin(angle)], axis=1).astype(jnp.bfloat16)

def phases(shift_y, shift_x, box):
    freq = jnp.arange(box * box, dtype=jnp.int32)
    freq_y = freq // box
    freq_x = freq % box
    phase = (freq_y[None, :] * shift_y[:, None] + freq_x[None, :] * shift_x[:, None]) % box
    angle = phase.astype(jnp.float32) * (2.0 * math.pi / box)
    return (jnp.cos(angle), jnp.sin(angle))

def evaluate(cross, shifts, box):
    volume = box * box
    cross_re = cross[:, :volume]
    cross_im = cross[:, volume:]
    columns = []
    for cand in range(shifts.shape[1]):
        cosine, sine = phases(shifts[:, cand, 0], shifts[:, cand, 1], box)
        columns.append(lax.optimization_barrier(jnp.sum(cross_re * cosine - cross_im * sine, axis=1)) / volume)
    return jnp.stack(columns, axis=1)

def steer(weights, shifts, box):
    phi_re = jnp.zeros((shifts.shape[0], box * box), jnp.float32)
    phi_im = jnp.zeros((shifts.shape[0], box * box), jnp.float32)
    for cand in range(shifts.shape[1]):
        cosine, sine = phases(shifts[:, cand, 0], shifts[:, cand, 1], box)
        phi_re = phi_re + weights[:, cand:cand + 1] * cosine
        phi_im = phi_im + weights[:, cand:cand + 1] * sine
    return (phi_re, phi_im)

def reference(particles, refs, orient, shifts, tilt, wedge):
    total = particles.shape[0]
    box = particles.shape[1]
    volume = box * box
    table = dft_table(box).astype(jnp.float32)
    blocks = total // P_DEV

    def one_block(carry, index):
        acc_spec, acc_weight = carry
        start = (index * P_DEV).astype(jnp.int32)
        block = lax.dynamic_slice_in_dim(particles, start, P_DEV, 0)
        block_orient = lax.dynamic_slice_in_dim(orient, start, P_DEV, 0)
        block_shifts = lax.dynamic_slice_in_dim(shifts, start, P_DEV, 0)
        block_tilt = lax.dynamic_slice_in_dim(tilt, start, P_DEV, 0)
        flat = block.reshape(P_DEV * box, volume).astype(jnp.float32)
        spectrum = jnp.dot(flat, table, precision=lax.Precision.HIGHEST).reshape(P_DEV, box, 2 * volume)
        fetched = jnp.take(refs, block_orient, axis=0).astype(jnp.float32)
        spec_re = spectrum[:, :, :volume]
        spec_im = spectrum[:, :, volume:]
        ref_re = fetched[:, :, :volume]
        ref_im = fetched[:, :, volume:]
        cross = jnp.concatenate([lax.optimization_barrier(jnp.sum(spec_re * ref_re + spec_im * ref_im, axis=1)), lax.optimization_barrier(jnp.sum(spec_im * ref_re - spec_re * ref_im, axis=1))], axis=1)
        corr = evaluate(cross, block_shifts, box)
        score = corr / math.sqrt(box)
        square = score * score
        weights = square / (4.0 + lax.optimization_barrier(jnp.sum(square, axis=1, keepdims=True)))
        mass = lax.optimization_barrier(jnp.sum(weights, axis=1))
        phi_re, phi_im = steer(weights, block_shifts, box)
        wedge_rows = jnp.take(wedge, block_tilt, axis=0)
        part_re = wedge_rows * (phi_re[:, None, :] * spec_re - phi_im[:, None, :] * spec_im)
        part_im = wedge_rows * (phi_re[:, None, :] * spec_im + phi_im[:, None, :] * spec_re)
        contrib = jnp.concatenate([part_re, part_im], axis=2).astype(jnp.bfloat16)
        contrib = lax.optimization_barrier(contrib).astype(jnp.float32)
        acc_spec = acc_spec.at[block_orient].add(contrib)
        acc_weight = acc_weight.at[block_orient].add(wedge_rows * mass[:, None, None])
        return ((acc_spec, acc_weight), weights)
    start_spec = jnp.zeros(refs.shape, jnp.float32)
    start_weight = jnp.zeros((refs.shape[0], box, volume), jnp.float32)
    (acc_spec, acc_weight), weight_blocks = lax.scan(one_block, (start_spec, start_weight), jnp.arange(blocks, dtype=jnp.int32))
    shift_weights = weight_blocks.reshape(total, shifts.shape[1])
    denom = acc_weight + 1.0
    fresh = jnp.concatenate([acc_spec[:, :, :volume] / denom, acc_spec[:, :, volume:] / denom], axis=2)
    sumsq = lax.optimization_barrier(jnp.sum(fresh * fresh, axis=(1, 2)))
    rms = jnp.sqrt(sumsq / (box * volume))
    new_refs = fresh / jnp.maximum(rms, 1.0)[:, None, None]
    return (new_refs, shift_weights)
```

```python
import math

import jax
import jax.numpy as jnp
import ml_dtypes
import numpy as np
from jax import lax
from jax.experimental import pallas as pl
from jax.experimental.pallas import tpu as pltpu
from jax.sharding import PartitionSpec as P

BOX = 32
VOLUME = BOX * BOX
TILTS = 16
CAP = 12
PEERS = 32
SLABS = 8
PLANES = 4
OWNED = 64
COUNT = 192
NCAND = 8
BINS = 81
GROUP = 4
WAVES = CAP // GROUP
CHUNK = GROUP * PLANES
ROWS = PEERS * CHUNK
BLOCK = 256
PER_BLOCK = BLOCK // CHUNK
LANES = 256

HIGH = lax.Precision.HIGHEST
MESH = pl.DeviceIdType.MESH
F32 = jnp.float32
BF16 = jnp.bfloat16


def unit_tables():
    freq = np.arange(BOX)
    phase = np.outer(freq, freq) % BOX
    cosine = np.cos(2 * np.pi * phase / BOX)
    sine = np.sin(2 * np.pi * phase / BOX)
    cosine[np.abs(cosine) < 1e-9] = 0
    sine[np.abs(sine) < 1e-9] = 0
    return cosine, sine


def axis_tables():
    cosine, sine = unit_tables()
    freq_y, freq_x = np.arange(VOLUME) // BOX, np.arange(VOLUME) % BOX
    tables = [cosine[:, freq_y], sine[:, freq_y], cosine[:, freq_x], sine[:, freq_x]]
    return np.stack(tables).astype(np.float32)


def bin_table():
    shift = np.arange(BINS)
    shift_y, shift_x = shift // 9 - 4, shift % 9 - 4
    freq_y, freq_x = np.arange(VOLUME) // BOX, np.arange(VOLUME) % BOX
    phase = (np.outer(shift_y, freq_y) + np.outer(shift_x, freq_x)) % BOX
    angle = 2 * np.pi * phase / BOX
    whole = np.concatenate([np.cos(angle), np.sin(angle)], axis=1).astype(np.float32)
    whole[np.abs(whole) < 1e-9] = 0
    high = whole.astype(ml_dtypes.bfloat16)
    low = (whole - high.astype(np.float32)).astype(ml_dtypes.bfloat16)
    rest = np.zeros((LANES - 3 * BINS, 2 * VOLUME), ml_dtypes.bfloat16)
    return np.concatenate([high, low, high, rest])


AXIS_TABLES = axis_tables()
BIN_TABLE = bin_table()


def dot(left, right, precision=None):
    return jnp.dot(left, right, preferred_element_type=F32, precision=precision)


def dot_nt(left, right, precision=None):
    return lax.dot_general(
        left, right, (((1,), (1,)), ((), ())), preferred_element_type=F32, precision=precision
    )


def dot_tn(left, right, precision=None):
    return lax.dot_general(
        left, right, (((0,), (0,)), ((), ())), preferred_element_type=F32, precision=precision
    )


def iota(shape, axis):
    return lax.broadcasted_iota(jnp.int32, shape, axis)


def twelfth(index):
    return (index * 43) >> 9


def hot(condition):
    return jnp.where(condition, 1.0, 0.0).astype(F32)


def kernel(
    part_ref,
    refs_ref,
    field_ref,
    wedge_ref,
    axis_ref,
    bins_ref,
    out_ref,
    weight_ref,
    table,
    send,
    recv,
    meta_send,
    meta_recv,
    spec,
    turned,
    corr,
    corr_all,
    square_all,
    back,
    back_send,
    back_recv,
    mixed,
    wedge3,
    wave_sent,
    wave_got,
    corr_sent,
    corr_got,
    one_sent,
    one_got,
):
    me = lax.axis_index("dom")
    slab = lax.axis_index("slab")

    barrier = pltpu.get_barrier_semaphore()

    def greet(step, carry):
        peer = lax.rem(me + step, PEERS)
        pl.semaphore_signal(barrier, inc=1, device_id={"dom": peer}, device_id_type=MESH)
        return carry

    lax.fori_loop(1, PEERS, greet, 0)

    def greet_slab(step, carry):
        peer = lax.rem(slab + step, SLABS)
        pl.semaphore_signal(barrier, inc=1, device_id={"slab": peer}, device_id_type=MESH)
        return carry

    lax.fori_loop(1, SLABS, greet_slab, 0)

    fields = field_ref[...]
    owner = fields[0:1] >> 6
    local = (fields[0:1] & (OWNED - 1)) + 1
    owner_hot = hot(iota((PEERS, LANES), 0) == owner)
    owner_hot16 = owner_hot.astype(BF16)
    before = dot(owner_hot16, hot(iota((LANES, LANES), 0) < iota((LANES, LANES), 1)).astype(BF16))
    rank = jnp.sum(before * owner_hot, axis=0, keepdims=True)

    lane = iota((128, LANES), 0)
    values = jnp.where(iota((16, LANES), 0) == 0, local, fields).astype(F32).astype(BF16)
    field_of = hot((twelfth(iota((128, 16), 0)) == iota((128, 16), 1)) & (iota((128, 16), 0) < 120))
    spread = dot(field_of.astype(BF16), values)
    slot_rank = (lane - 12 * twelfth(lane)).astype(F32)
    spread = jnp.where(slot_rank == rank, spread, 0.0)
    meta = dot_nt(owner_hot16, spread.astype(BF16))
    for peer in range(PEERS):
        meta_send[peer] = meta[peer : peer + 1]

    pair = jnp.where(
        iota((8, LANES), 0) == 0,
        owner.astype(F32),
        jnp.where(iota((8, LANES), 0) == 1, rank, 0.0),
    )
    repeat = hot((iota((LANES, COUNT * PLANES), 1) >> 2) == iota((LANES, COUNT * PLANES), 0))
    pair4 = dot(pair.astype(BF16), repeat.astype(BF16))
    plane4 = (iota((1, COUNT * PLANES), 1) & 3).astype(F32)
    code = (pair4[0:1] * CAP + pair4[1:2]) * PLANES + plane4

    def pack(wave):
        def pack_block(block, carry):
            row = iota((BLOCK, COUNT * PLANES), 0)
            dest = block * PER_BLOCK + (row >> 4)
            row_code = (dest * CAP + wave * GROUP) * PLANES + (row & 15)
            chosen = hot(row_code.astype(F32) == code).astype(BF16)
            start = pl.multiple_of(block * BLOCK, BLOCK)
            send[wave, pl.ds(start, BLOCK), :] = dot(chosen, part_ref[...]).astype(BF16)
            return carry

        lax.fori_loop(0, ROWS // BLOCK, pack_block, 0)

    def chunk(index):
        return pl.ds(pl.multiple_of(index * CHUNK, CHUNK), CHUNK)

    def send_wave(wave):
        def one(step, carry):
            peer = lax.rem(me + step, PEERS)
            pltpu.make_async_remote_copy(
                src_ref=send.at[wave, chunk(peer), :],
                dst_ref=recv.at[wave, chunk(me), :],
                send_sem=wave_sent.at[wave],
                recv_sem=wave_got.at[wave],
                device_id={"dom": peer},
                device_id_type=MESH,
            ).start()
            return carry

        lax.fori_loop(1, PEERS, one, 0)

    def wave_copy(wave):
        others = pl.ds(0, ROWS - CHUNK)
        return pltpu.make_async_remote_copy(
            src_ref=send.at[wave, others, :],
            dst_ref=recv.at[wave, others, :],
            send_sem=wave_sent.at[wave],
            recv_sem=wave_got.at[wave],
            device_id={"dom": me},
            device_id_type=MESH,
        )

    def small_copy(source, target, slot, axis, peer):
        return pltpu.make_async_remote_copy(
            src_ref=source,
            dst_ref=target,
            send_sem=one_sent.at[slot],
            recv_sem=one_got.at[slot],
            device_id={axis: peer},
            device_id_type=MESH,
        )

    pack(0)
    pack(1)
    pl.semaphore_wait(barrier, PEERS - 1 + SLABS - 1)

    def send_meta(step, carry):
        peer = lax.rem(me + step, PEERS)
        small_copy(meta_send.at[peer], meta_recv.at[me], 0, "dom", peer).start()
        return carry

    lax.fori_loop(1, PEERS, send_meta, 0)
    send_wave(0)
    pack(2)
    send_wave(1)

    def fill(row, carry):
        cos_y = axis_ref[0, pl.ds(row, 1), :]
        sin_y = axis_ref[1, pl.ds(row, 1), :]
        cos_x = axis_ref[2]
        sin_x = axis_ref[3]
        start = pl.multiple_of(row * BOX, BOX)
        table[pl.ds(start, BOX), 0:VOLUME] = (cos_y * cos_x - sin_y * sin_x).astype(BF16)
        table[pl.ds(start, BOX), VOLUME:] = (-(sin_y * cos_x + cos_y * sin_x)).astype(BF16)
        return carry

    lax.fori_loop(0, BOX, fill, 0)
    send_wave(2)

    whole = wedge_ref[...]
    first = whole.astype(BF16)
    rest = whole - first.astype(F32)
    second = rest.astype(BF16)
    third = (rest - second.astype(F32)).astype(BF16)
    wedge3[0:64] = first
    wedge3[64:128] = second
    wedge3[128:192] = third
    wedge3[192:256] = jnp.zeros((64, VOLUME), BF16)

    for wave in range(WAVES):
        recv[wave, chunk(me), :] = send[wave, chunk(me), :]
    meta_recv[me] = meta_send[me]
    out_ref[...] = jnp.zeros_like(out_ref)
    mixed[...] = jnp.zeros_like(mixed)
    back[...] = jnp.zeros_like(back)

    others = pl.ds(0, PEERS - 1)
    small_copy(meta_send.at[others], meta_recv.at[others], 0, "dom", me).wait_recv()
    held = meta_recv[...].reshape(PEERS, 128).astype(BF16)

    def block_meta(wave, block):
        row = iota((BLOCK, PEERS), 0)
        take = hot(block * PER_BLOCK + (row >> 4) == iota((BLOCK, PEERS), 1))
        every = dot(take.astype(BF16), held)
        lane = iota((BLOCK, 128), 1)
        place = wave * GROUP + ((iota((BLOCK, 128), 0) & 15) >> 2)
        mine = jnp.where(lane - 12 * twelfth(lane) == place, every, 0.0)
        pick = hot((twelfth(iota((16, 128), 1)) == iota((16, 128), 0)) & (iota((16, 128), 1) < 120))
        return dot_nt(pick.astype(BF16), mine.astype(BF16))

    sub = iota((LANES, BLOCK), 0)
    plane_row = (iota((1, BLOCK), 1) & 3).astype(F32)
    part = hot(sub >= BINS) + hot(sub >= 2 * BINS)
    bin_of = jnp.where(sub < 3 * BINS, sub.astype(F32) - BINS * part, -1.0)
    bin_score = jnp.where(sub < 2 * BINS, bin_of, -1.0)

    def orient_hot(meta_t):
        return hot(sub.astype(F32) == (meta_t[0:1] - 1.0) * PLANES + plane_row)

    def slots_of(block):
        return iota((BLOCK, 128), 1) == block * (BLOCK // PLANES) + (iota((BLOCK, 128), 0) >> 2)

    def columns(index, offset=0):
        return pl.ds(pl.multiple_of(index * LANES + offset, LANES), LANES)

    def run_wave(wave, carry):
        wave_copy(wave).wait_recv()
        corr[...] = jnp.zeros_like(corr)

        def score_block(block, carry):
            meta_t = block_meta(wave, block)
            chosen = orient_hot(meta_t).T.astype(BF16)
            rows = pl.ds(pl.multiple_of(block * BLOCK, BLOCK), BLOCK)
            turned[...] = jnp.zeros_like(turned)

            def score_columns(index, carry):
                re, im = columns(index), columns(index, VOLUME)
                data = recv[wave, rows, :]
                s_re = dot(data, table[:, re])
                s_im = dot(data, table[:, im])
                spec[wave, rows, re] = s_re
                spec[wave, rows, im] = s_im
                r_re = dot(chosen, refs_ref[:, re])
                r_im = dot(chosen, refs_ref[:, im])
                q_re = s_re * r_re + s_im * r_im
                q_im = s_re * r_im - s_im * r_re
                total = turned[...]
                for value, where in ((q_re, re), (q_im, im)):
                    high = value.astype(BF16)
                    low = (value - high.astype(F32)).astype(BF16)
                    total += dot_nt(bins_ref[:, where], high) + dot_nt(bins_ref[:, where], low)
                turned[...] = total
                return carry

            lax.fori_loop(0, VOLUME // LANES, score_columns, 0)
            total = turned[...]
            scores = jnp.zeros((NCAND, BLOCK), F32)
            for cand in range(NCAND):
                one = jnp.sum(
                    jnp.where(bin_score == meta_t[2 + cand : 3 + cand], total, 0.0),
                    axis=0,
                    keepdims=True,
                )
                scores = jnp.where(iota((NCAND, BLOCK), 0) == cand, one, scores)
            corr[...] += dot(scores, hot(slots_of(block)), HIGH)
            return carry

        lax.fori_loop(0, ROWS // BLOCK, score_block, 0)
        corr_all[wave, slab] = corr[...]

        def corr_copy(source, target, peer):
            return pltpu.make_async_remote_copy(
                src_ref=source,
                dst_ref=target,
                send_sem=corr_sent.at[wave],
                recv_sem=corr_got.at[wave],
                device_id={"slab": peer},
                device_id_type=MESH,
            )

        def send_corr(step, carry):
            peer = lax.rem(slab + step, SLABS)
            corr_copy(corr_all.at[wave, slab], corr_all.at[wave, slab], peer).start()
            return carry

        lax.fori_loop(1, SLABS, send_corr, 0)
        seven = pl.ds(0, SLABS - 1)
        corr_copy(corr_all.at[wave, seven], corr_all.at[wave, seven], slab).wait()

        total = jnp.zeros((NCAND, 128), F32)
        for peer in range(SLABS):
            total += corr_all[wave, peer]
        score = total / VOLUME / math.sqrt(BOX)
        square = score * score
        weights = square / (4.0 + jnp.sum(square, axis=0, keepdims=True))

        lane = iota((128, 128), 0)
        cand_of = hot(twelfth(iota((128, NCAND), 0)) == iota((128, NCAND), 1))
        wide = dot(cand_of, weights, HIGH)
        place = (iota((128, 128), 1) & 3) + wave * GROUP
        wide = jnp.where(lane - 12 * twelfth(lane) == place, wide, 0.0)
        fold = hot((iota((128, 128), 0) >> 2) == iota((128, 128), 1))
        back[...] += dot(wide, fold, HIGH)

        def steer_block(block, carry):
            meta_t = block_meta(wave, block)
            rows = pl.ds(pl.multiple_of(block * BLOCK, BLOCK), BLOCK)
            chosen_t = orient_hot(meta_t).astype(BF16)
            slot_t = iota((128, BLOCK), 0) == block * (BLOCK // PLANES) + (iota((128, BLOCK), 1) >> 2)
            weight_t = dot(weights, hot(slot_t), HIGH)
            mass = jnp.sum(weight_t, axis=0, keepdims=True)
            binned = jnp.zeros((LANES, BLOCK), F32)
            for cand in range(NCAND):
                binned += jnp.where(
                    bin_of == meta_t[2 + cand : 3 + cand], weight_t[cand : cand + 1], 0.0
                )
            high = binned.astype(BF16).astype(F32)
            binned = jnp.where(sub < 2 * BINS, high, binned - high).T.astype(BF16)
            tilt_row = meta_t[1:2] * PLANES + plane_row
            tilt_hit = (sub & 63).astype(F32) == tilt_row
            tilt_hot = hot(tilt_hit & (sub < 192)).T.astype(BF16)
            mass_high = mass.astype(BF16).astype(F32)
            mass_part = jnp.where(sub < 64, mass_high, mass - mass_high)
            share = jnp.where(tilt_hit, mass_part, 0.0)[0:128].T.astype(BF16)
            mixed[...] += dot(chosen_t, share)

            def steer_columns(index, carry):
                re, im = columns(index), columns(index, VOLUME)
                phi_re = dot(binned, bins_ref[:, re])
                phi_im = dot(binned, bins_ref[:, im])
                scale = dot(tilt_hot, wedge3[:, re])
                s_re = spec[wave, rows, re]
                s_im = spec[wave, rows, im]
                part_re = scale * (phi_re * s_re - phi_im * s_im)
                part_im = scale * (phi_re * s_im + phi_im * s_re)
                out_ref[:, re] += dot(chosen_t, part_re.astype(BF16))
                out_ref[:, im] += dot(chosen_t, part_im.astype(BF16))
                return carry

            lax.fori_loop(0, VOLUME // LANES, steer_columns, 0)
            return carry

        lax.fori_loop(0, ROWS // BLOCK, steer_block, 0)
        return carry

    lax.fori_loop(0, WAVES, run_wave, 0)

    answer = back[...].T
    for peer in range(PEERS):
        back_send[peer] = answer[peer : peer + 1]

    def send_back(step, carry):
        peer = lax.rem(me + step, PEERS)
        small_copy(back_send.at[peer], back_recv.at[me], 1, "dom", peer).start()
        return carry

    lax.fori_loop(1, PEERS, send_back, 0)
    back_recv[me] = back_send[me]

    halves = mixed[...]
    halves = halves + pltpu.roll(halves, 64, 1)
    mixed_high = halves.astype(BF16)
    mixed_low = (halves - mixed_high.astype(F32)).astype(BF16)
    squares = jnp.zeros((LANES, 128), F32)
    for index in range(VOLUME // LANES):
        re = slice(index * LANES, (index + 1) * LANES)
        im = slice(VOLUME + index * LANES, VOLUME + (index + 1) * LANES)
        weight = dot(mixed_high, wedge3[0:128, re]) + dot(mixed_low, wedge3[0:128, re])
        over = 1.0 / (weight + 1.0)
        for where in (re, im):
            fresh = out_ref[:, where] * over
            out_ref[:, where] = fresh
            power = fresh * fresh
            squares += power[:, 0:128] + power[:, 128:256]
    power = jnp.sum(squares.T, axis=0, keepdims=True)
    power = jnp.broadcast_to(power, (8, LANES))
    fold = hot((iota((LANES, 128), 0) >> 2) == iota((LANES, 128), 1))
    square_all[slab] = dot(power, fold, HIGH)

    def send_square(step, carry):
        peer = lax.rem(slab + step, SLABS)
        small_copy(square_all.at[slab], square_all.at[slab], 2, "slab", peer).start()
        return carry

    lax.fori_loop(1, SLABS, send_square, 0)

    small_copy(back_send.at[others], back_recv.at[others], 1, "dom", me).wait()
    answers = back_recv[...].reshape(PEERS, 128)
    found = dot_tn(answers, owner_hot, HIGH)
    found = jnp.where(slot_rank == rank, found, 0.0)
    gather = hot(twelfth(iota((NCAND, 128), 1)) == iota((NCAND, 128), 0))
    weight_ref[...] = dot(gather, found, HIGH)

    seven = pl.ds(0, SLABS - 1)
    small_copy(square_all.at[seven], square_all.at[seven], 2, "slab", slab).wait()
    total = jnp.zeros((8, 128), F32)
    for peer in range(SLABS):
        total += square_all[peer]
    rms = jnp.sqrt(total / (BOX * VOLUME))
    scale = 1.0 / jnp.maximum(rms, 1.0)
    unfold = hot((iota((128, LANES), 1) >> 2) == iota((128, LANES), 0))
    scale = dot(scale, unfold, HIGH)
    scale = jnp.broadcast_to(scale[0:1], (128, LANES)).T[:, 0:1]
    out_ref[...] = out_ref[...] * scale

    small_copy(meta_send.at[others], meta_recv.at[others], 0, "dom", me).wait_send()
    for wave in range(WAVES):
        wave_copy(wave).wait_send()


def shards(particles, refs, orient, shifts, tilt, wedge):
    steps = jnp.transpose(shifts, (1, 2, 0)) + 4
    bins = steps[:, 0] * 9 + steps[:, 1]
    fields = jnp.concatenate(
        [orient[None], tilt[None], bins, jnp.zeros((6, COUNT), jnp.int32)], axis=0
    )
    fields = jnp.pad(fields, ((0, 0), (0, LANES - COUNT)), constant_values=4096)
    vmem = pl.BlockSpec(memory_space=pltpu.VMEM)
    scratch = [
        pltpu.VMEM((VOLUME, 2 * VOLUME), BF16),
        pltpu.VMEM((WAVES, ROWS, VOLUME), BF16),
        pltpu.VMEM((WAVES, ROWS, VOLUME), BF16),
        pltpu.VMEM((PEERS, 1, 128), F32),
        pltpu.VMEM((PEERS, 1, 128), F32),
        pltpu.VMEM((WAVES, ROWS, 2 * VOLUME), F32),
        pltpu.VMEM((LANES, BLOCK), F32),
        pltpu.VMEM((NCAND, 128), F32),
        pltpu.VMEM((WAVES, SLABS, NCAND, 128), F32),
        pltpu.VMEM((SLABS, 8, 128), F32),
        pltpu.VMEM((128, 128), F32),
        pltpu.VMEM((PEERS, 1, 128), F32),
        pltpu.VMEM((PEERS, 1, 128), F32),
        pltpu.VMEM((LANES, 128), F32),
        pltpu.VMEM((LANES, VOLUME), BF16),
        pltpu.SemaphoreType.DMA((WAVES,)),
        pltpu.SemaphoreType.DMA((WAVES,)),
        pltpu.SemaphoreType.DMA((WAVES,)),
        pltpu.SemaphoreType.DMA((WAVES,)),
        pltpu.SemaphoreType.DMA((3,)),
        pltpu.SemaphoreType.DMA((3,)),
    ]
    new_refs, weights = pl.pallas_call(
        kernel,
        out_shape=(
            jax.ShapeDtypeStruct((OWNED * PLANES, 2 * VOLUME), F32),
            jax.ShapeDtypeStruct((NCAND, LANES), F32),
        ),
        in_specs=[vmem] * 6,
        out_specs=(vmem, vmem),
        scratch_shapes=scratch,
        compiler_params=pltpu.CompilerParams(
            collective_id=0, has_side_effects=True, vmem_limit_bytes=60 << 20
        ),
        name="refine",
    )(
        particles.reshape(COUNT * PLANES, VOLUME),
        refs.reshape(OWNED * PLANES, 2 * VOLUME),
        fields,
        wedge.reshape(TILTS * PLANES, VOLUME),
        jnp.asarray(AXIS_TABLES),
        jnp.asarray(BIN_TABLE),
    )
    return new_refs.reshape(OWNED, PLANES, 2 * VOLUME), weights[:, :COUNT].T


def solution(mesh):
    placed = (
        P("dom", "slab", None),
        P("dom", "slab", None),
        P("dom"),
        P("dom", None, None),
        P("dom"),
        P(None, "slab", None),
    )
    return jax.shard_map(
        shards,
        mesh=mesh,
        in_specs=placed,
        out_specs=(P("dom", "slab", None), P("dom", None)),
        check_vma=False,
    )
```
